32 devices in a mesh: row: 4 (over x, core), col: 8 (over z, y).
Axes of the slice: x: 2, y: 2, z: 4, core: 2. Of those that a mesh axis runs over, the one named last changes fastest.
Arguments:
- latent: bfloat16 [24, 96, 1536], P('row', 'col'), may hold values from -6 to 6
- attn_shift: float32 [1536], replicated, may hold values from -3 to 3
- attn_scale: float32 [1536], replicated, may hold values from -2.5 to 2.5
- attn_gate: float32 [1536], replicated, may hold values from 1 to 3
- final_shift: float32 [1536], replicated, may hold values from -3 to 3
- final_scale: float32 [1536], replicated, may hold values from -2.5 to 2.5
- q_weight: bfloat16 [1536, 768], replicated, may hold values from -2 to 2
- k_weight: bfloat16 [1536, 768], replicated, may hold values from -2 to 2
- v_weight: bfloat16 [1536, 768], replicated, may hold values from -0.15625 to 0.15625
- o_weight: bfloat16 [768, 1536], replicated, may hold values from -0.21875 to 0.21875
- out_weight: bfloat16 [1536, 64], replicated, may hold values from -0.15625 to 0.15625
- neighbour_mask: int32 [4, 8, 4], P('row', 'col'), may hold values 0 or 1
- blend_weight: float32 [32, 128], P('row', 'col'), may hold values from 0.25 to 4
Outputs:
- latent_out: float32 [24, 6144], P('row', 'col')
The draws below stay inside these ranges and needn't reach their ends.
All inputs are finite; a program needn't handle non-finite values. No bound on the sum of `neighbour_mask` on one device may be relied on, other than what follows from the above.
Results may differ from the reference program's by a relative error of at most 0.008.
The reference program's roundings to bfloat16 on the way count: a program that leaves them out, or rounds other values in their place, can miss the bound.
Values may be sent and summed in bfloat16 or wider, within the bound.
No kernel may reach another device: no remote copies, remote signals or barrier semaphores. Data moves between devices by JAX's collectives and lax.ppermute only.
A program may use at most 64 MiB of HBM per device.

```python
import math
import jax
import jax.numpy as jnp
from jax import lax

D = 1536
HD = 64
HEADS = 12
P_SIZE = 64
TH = 6
TW = 12
EH = 2
EW = 4
WH = 8
WW = 16
HGRID = 24
WGRID = 96
N_ROW = 4
N_COL = 8


def qk_pair(key):
    width_attn = HEADS * HD
    scale_std = 1.5 / D ** 0.5
    query_part = jax.random.normal(jax.random.fold_in(key, 11), (D, width_attn), jnp.float32) * scale_std
    key_part = jax.random.normal(jax.random.fold_in(key, 12), (D, width_attn), jnp.float32) * scale_std
    return (jnp.clip(query_part, -2.0, 2.0), jnp.clip(key_part, -2.0, 2.0))


def draw_q_weight(key, part):
    return qk_pair(key)[0].astype(jnp.bfloat16)


def draw_k_weight(key, part):
    return qk_pair(key)[1].astype(jnp.bfloat16)


def touch_ends(array, own_key, low, high):
    index_at = [jax.random.randint(jax.random.fold_in(own_key, axis), (), 0, length) for axis, length in enumerate(array.shape)]
    main_axis = array.shape.index(max(array.shape))
    next_to = index_at[:main_axis] + [(index_at[main_axis] + 1) % array.shape[main_axis]] + index_at[main_axis + 1:]
    return array.at[tuple(index_at)].set(low).at[tuple(next_to)].set(high)


def block_scale(key, dims, pieces, least, largest):
    loudness, own = 1.0, jax.random.fold_in(key, 6)
    for position, parts in pieces:
        draws = jnp.exp(jax.random.uniform(jax.random.fold_in(own, position), (parts,), jnp.float32, least / len(pieces), largest / len(pieces)))
        loudness = loudness * jnp.repeat(draws, dims[position] // parts).reshape([-1 if axis == position else 1 for axis in range(len(dims))])
    return loudness


def noise(key, dims, scale, reach, shards=(), kind=jnp.bfloat16):
    values = scale * jax.random.normal(key, dims, jnp.float32)
    if shards:
        values = values * block_scale(key, dims, shards, -0.22, 0.18)
    return jnp.clip(values, -reach, reach).astype(kind)


def setup_inputs(seed: int = 0) -> dict:
    key_list = jax.random.split(jax.random.key(seed), 14)
    latent = noise(key_list[0], (HGRID, WGRID, D), 1.0, 6.0, ((0, 4), (1, 8)))
    attn_shift = noise(key_list[1], (D,), 0.5, 3.0, (), jnp.float32)
    attn_scale = noise(key_list[2], (D,), 0.3, 2.5, (), jnp.float32)
    attn_gate = jnp.clip(jax.random.uniform(key_list[3], (D,), jnp.float32, 1.0, 3.0), 1.0, 3.0)
    final_shift = noise(key_list[4], (D,), 0.5, 3.0, (), jnp.float32)
    final_scale = noise(key_list[5], (D,), 0.3, 2.5, (), jnp.float32)
    q_weight = draw_q_weight(jax.random.fold_in(key_list[13], 71), 0)
    k_weight = draw_k_weight(jax.random.fold_in(key_list[13], 71), 0)
    v_weight = noise(key_list[8], (D, HEADS * HD), D ** -0.5, 0.15625)
    o_weight = noise(key_list[9], (HEADS * HD, D), (HEADS * HD) ** -0.5, 0.21875)
    out_weight = noise(key_list[10], (D, P_SIZE), D ** -0.5, 0.15625)
    neighbour_mask = touch_ends((jax.random.randint(key_list[11], (N_ROW, N_COL, 4), 0, 4) < 3).astype(jnp.int32), jax.random.fold_in(key_list[11], 1), 0, 1)
    blend_weight = jnp.clip(jnp.exp(math.log(4.0) - 2.7725887 * jax.random.uniform(key_list[12], (N_ROW * WH, N_COL * WW), jnp.float32) ** block_scale(key_list[12], (N_ROW * WH, N_COL * WW), ((0, 4), (1, 8)), -0.2, 0.2)), 0.25, 4.0)
    return dict(latent=latent, attn_shift=attn_shift, attn_scale=attn_scale, attn_gate=attn_gate, final_shift=final_shift, final_scale=final_scale, q_weight=q_weight, k_weight=k_weight, v_weight=v_weight, o_weight=o_weight, out_weight=out_weight, neighbour_mask=neighbour_mask, blend_weight=blend_weight)


EPSILON = 1e-06

def layer_norm(features):
    center = features - lax.optimization_barrier(jnp.mean(features, axis=-1, keepdims=True))
    spread = lax.optimization_barrier(jnp.mean(center * center, axis=-1, keepdims=True))
    return center * lax.rsqrt(spread + EPSILON)

def pad_block(part_block):
    widths = [(0, 0), (0, 0), (0, TH - part_block.shape[2]), (0, TW - part_block.shape[3])]
    widths = widths + [(0, 0)] * (part_block.ndim - 4)
    return jnp.pad(part_block, widths)

def fold_windows(stacked):
    left_win = jnp.roll(stacked, 1, axis=1)
    upper_win = jnp.roll(stacked, 1, axis=0)
    corner_win = jnp.roll(upper_win, 1, axis=1)
    total_sum = stacked[:, :, :TH, :TW]
    total_sum = total_sum + pad_block(left_win[:, :, :TH, TW:])
    total_sum = total_sum + pad_block(upper_win[:, :, TH:, :TW])
    total_sum = total_sum + pad_block(corner_win[:, :, TH:, TW:])
    return total_sum

def reference(latent, attn_shift, attn_scale, attn_gate, final_shift, final_scale, q_weight, k_weight, v_weight, o_weight, out_weight, neighbour_mask, blend_weight):
    width_attn = HEADS * HD
    tokens_win = WH * WW
    padded = jnp.concatenate([latent, latent[:EH]], axis=0)
    padded = jnp.concatenate([padded, padded[:, :EW]], axis=1)

    def window_at(index_win):
        row_idx = (index_win // N_COL).astype(jnp.int32)
        col_idx = (index_win % N_COL).astype(jnp.int32)
        zero_idx = jnp.zeros((), jnp.int32)
        window_block = lax.dynamic_slice(padded, (row_idx * TH, col_idx * TW, zero_idx), (WH, WW, D))
        return (window_block.reshape(tokens_win, D), row_idx, col_idx)

    def project(index_win):
        window_block, row_idx, col_idx = window_at(index_win)
        normed = (layer_norm(window_block.astype(jnp.float32)) * (1.0 + attn_scale) + attn_shift).astype(jnp.bfloat16)
        queries = jnp.dot(normed, q_weight, preferred_element_type=jnp.float32).astype(jnp.bfloat16)
        key_rows = jnp.dot(normed, k_weight, preferred_element_type=jnp.float32).astype(jnp.bfloat16)
        values = jnp.dot(normed, v_weight, preferred_element_type=jnp.float32).astype(jnp.bfloat16)
        return (queries, key_rows, values)
    indices = jnp.arange(N_ROW * N_COL, dtype=jnp.int32)
    all_q, all_k, all_v = lax.map(project, indices)

    def attend(index_win):
        window_block, row_idx, col_idx = window_at(index_win)
        neighbours = [(row_idx - 1) % N_ROW * N_COL + col_idx, (row_idx + 1) % N_ROW * N_COL + col_idx, row_idx * N_COL + (col_idx - 1) % N_COL, row_idx * N_COL + (col_idx + 1) % N_COL]
        context_k = jnp.concatenate([all_k[index_win]] + [all_k[other] for other in neighbours], axis=0)
        context_v = jnp.concatenate([all_v[index_win]] + [all_v[other] for other in neighbours], axis=0)
        live_flags = neighbour_mask[row_idx, col_idx].astype(jnp.int32)
        live_all = jnp.concatenate([jnp.ones((1,), jnp.int32), live_flags])
        live_rep = jnp.repeat(live_all, tokens_win)
        query_h = all_q[index_win].astype(jnp.float32).reshape(tokens_win, HEADS, HD)
        key_h = context_k.astype(jnp.float32).reshape(5 * tokens_win, HEADS, HD)
        value_h = context_v.astype(jnp.float32).reshape(5 * tokens_win, HEADS, HD)
        scores = jnp.einsum('qhd,khd->hqk', query_h, key_h) / HD ** 0.5
        scores = jnp.where(live_rep[None, None, :] > 0, scores, -1e+30)
        weights = jax.nn.softmax(scores, axis=-1).astype(jnp.bfloat16)
        attended = jnp.einsum('hqk,khd->qhd', weights.astype(jnp.float32), value_h)
        attended = attended.reshape(tokens_win, width_attn).astype(jnp.bfloat16)
        mixed_sum = window_block.astype(jnp.float32) + attn_gate * jnp.dot(attended, o_weight, preferred_element_type=jnp.float32)
        final_normed = (layer_norm(mixed_sum) * (1.0 + final_scale) + final_shift).astype(jnp.bfloat16)
        patch = jnp.dot(final_normed, out_weight, preferred_element_type=jnp.float32)
        blend_block = lax.dynamic_slice(blend_weight, (row_idx * WH, col_idx * WW), (WH, WW))
        numerator = blend_block[:, :, None] * patch.reshape(WH, WW, P_SIZE)
        return (numerator, blend_block)
    numerators, blends = lax.map(attend, indices)
    numerators = numerators.reshape(N_ROW, N_COL, WH, WW, P_SIZE)
    blends = blends.reshape(N_ROW, N_COL, WH, WW)
    num_total = fold_windows(numerators)
    weight_total = fold_windows(blends)
    latent_out = num_total / weight_total[..., None]
    return latent_out.transpose(0, 2, 1, 3, 4).reshape(N_ROW * TH, N_COL * TW * P_SIZE)
```

```python
import functools

import jax
import jax.numpy as jnp
from jax import lax
from jax.experimental import pallas as pl
from jax.experimental.pallas import tpu as pltpu
from jax.sharding import PartitionSpec as P

D = 1536
HD = 64
HEADS = 12
P_SIZE = 64
TH = 6
TW = 12
EH = 2
EW = 4
WH = 8
WW = 16
AD = HEADS * HD
PAIRS = HEADS // 2
OWN = WH * WW
SIDE = WH * TW
KEYS = OWN + 4 * SIDE
LANES = 128

EPSILON = 1e-06
BLOCKED = -1e30
F32 = jnp.float32
BF16 = jnp.bfloat16


def fetch(block, down, right):
    n_row, n_col = lax.axis_size("row"), lax.axis_size("col")
    route = [
        (((r + down) % n_row) * n_col + (c + right) % n_col, r * n_col + c)
        for r in range(n_row)
        for c in range(n_col)
    ]
    return lax.ppermute(block, ("row", "col"), route)


def layer_norm(features, scale, shift):
    center = features - jnp.mean(features, axis=-1, keepdims=True)
    spread = jnp.mean(center * center, axis=-1, keepdims=True)
    normed = center * lax.rsqrt(spread + EPSILON)
    return (normed * (1.0 + scale) + shift).astype(BF16)


def dot(a, b):
    return jnp.dot(a, b, preferred_element_type=F32)


def pack_kernel(x_ref, right_ref, lower_ref, corner_ref):
    for r in range(TH):
        right_ref[EW * r : EW * (r + 1)] = x_ref[r, :EW]
    for r in range(EH):
        lower_ref[TW * r : TW * (r + 1)] = x_ref[r]
        corner_ref[EW * r : EW * (r + 1)] = x_ref[r, :EW]


def assemble_kernel(x_ref, right_ref, lower_ref, corner_ref, win_ref, up_ref, down_ref, left_ref, out_ref):
    for r in range(WH):
        if r < TH:
            body, tail = x_ref[r], right_ref[EW * r : EW * (r + 1)]
        else:
            k = r - TH
            body, tail = lower_ref[TW * k : TW * (k + 1)], corner_ref[EW * k : EW * (k + 1)]
        row = jnp.concatenate([body, tail], axis=0)
        win_ref[WW * r : WW * (r + 1)] = row
        if r >= EH:
            up_ref[WW * (r - EH) : WW * (r - EH + 1)] = row
        if r < TH:
            down_ref[WW * r : WW * (r + 1)] = row
        left_ref[TW * r : TW * (r + 1)] = row[EW:]
        out_ref[TW * r : TW * (r + 1)] = body


def own_kernel(win_ref, scale_ref, shift_ref, qw_ref, kw_ref, vw_ref, q_ref, k_ref, v_ref):
    normed = layer_norm(win_ref[...].astype(F32), scale_ref[...], shift_ref[...])
    q_ref[...] = dot(normed, qw_ref[...]).astype(BF16)
    k_ref[...] = dot(normed, kw_ref[...]).astype(BF16)
    v_ref[...] = dot(normed, vw_ref[...]).astype(BF16)


def rest_kernel(
    mask_ref,
    win_ref,
    q_ref,
    k_ref,
    v_ref,
    up_ref,
    down_ref,
    left_ref,
    right_ref,
    scale_ref,
    shift_ref,
    gate_ref,
    fscale_ref,
    fshift_ref,
    kw_ref,
    vw_ref,
    ow_ref,
    pw_ref,
    blend_ref,
    kept_ref,
    spill_e_ref,
    spill_s_ref,
    spill_c_ref,
    normed_ref,
    keys_ref,
    vals_ref,
    att_ref,
):
    for j, side in enumerate((up_ref, down_ref, left_ref, right_ref)):
        normed_ref[SIDE * j : SIDE * (j + 1)] = layer_norm(
            side[...].astype(F32), scale_ref[...], shift_ref[...]
        )
    normed = normed_ref[...]
    keys_ref[:OWN] = k_ref[...]
    keys_ref[OWN:] = dot(normed, kw_ref[...]).astype(BF16)
    values = dot(normed, vw_ref[...]).astype(BF16)
    for p in range(PAIRS):
        vals_ref[p, :OWN, :LANES] = v_ref[:, LANES * p : LANES * (p + 1)]
        vals_ref[p, OWN:, :LANES] = values[:, LANES * p : LANES * (p + 1)]
        vals_ref[p, :, LANES:] = jnp.ones((KEYS, LANES), BF16)

    live = [mask_ref[j] for j in range(4)]
    token = lax.broadcasted_iota(jnp.int32, (1, OWN), 1)
    row, col = token // WW, token % WW
    times = (
        1
        + jnp.where(row < EH, live[0], 0)
        + jnp.where(row >= TH, live[1], 0)
        + jnp.where(col < EW, live[2], 0)
        + jnp.where(col >= TW, live[3], 0)
    ).astype(F32)
    place = lax.broadcasted_iota(jnp.int32, (1, KEYS), 1)
    shut = jnp.zeros((1, KEYS), F32)
    for j in range(4):
        inside = (place >= OWN + SIDE * j) & (place < OWN + SIDE * (j + 1))
        shut = jnp.where(inside & (live[j] == 0), BLOCKED, shut)
    times = jnp.concatenate([times, jnp.ones((1, KEYS - OWN), F32)], axis=1)
    lane = lax.broadcasted_iota(jnp.int32, (OWN, LANES), 1)
    first = lane < HD
    zero = jnp.zeros((OWN, LANES), BF16)
    for p in range(PAIRS):
        q = q_ref[:, LANES * p : LANES * (p + 1)] * BF16(HD**-0.5)
        both = jnp.concatenate([jnp.where(first, q, zero), jnp.where(first, zero, q)], axis=0)
        scores = lax.dot_general(
            both,
            keys_ref[:, LANES * p : LANES * (p + 1)],
            (((1,), (1,)), ((), ())),
            preferred_element_type=F32,
        )
        scores = scores + shut
        top = jnp.max(scores, axis=-1, keepdims=True)
        weights = (jnp.exp(scores - top) * times).astype(BF16)
        out = dot(weights, vals_ref[p])
        out = out[:, :LANES] / out[:, LANES:]
        att_ref[:, LANES * p : LANES * (p + 1)] = jnp.where(first, out[:OWN], out[OWN:]).astype(BF16)

    mixed = win_ref[...].astype(F32) + gate_ref[...] * dot(att_ref[...], ow_ref[...])
    final = layer_norm(mixed, fscale_ref[...], fshift_ref[...])
    patch = dot(final, pw_ref[...])
    spread = jnp.concatenate(
        [jnp.broadcast_to(blend_ref[r : r + 1], (WW, WW)) for r in range(WH)], axis=0
    )
    own_row = lax.broadcasted_iota(jnp.int32, (OWN, WW), 0) % WW
    own_col = lax.broadcasted_iota(jnp.int32, (OWN, WW), 1)
    b = jnp.sum(jnp.where(own_row == own_col, spread, 0.0), axis=1, keepdims=True)
    both = jnp.concatenate([b * patch, jnp.broadcast_to(b, (OWN, P_SIZE))], axis=1)
    for r in range(WH):
        at = WW * r
        if r < TH:
            kept_ref[TW * r : TW * (r + 1)] = both[at : at + TW]
            spill_e_ref[EW * r : EW * (r + 1)] = both[at + TW : at + WW]
        else:
            k = r - TH
            spill_s_ref[TW * k : TW * (k + 1)] = both[at : at + TW]
            spill_c_ref[EW * k : EW * (k + 1)] = both[at + TW : at + WW]


def blend_kernel(kept_ref, left_ref, upper_ref, corner_ref, out_ref):
    for y in range(TH):
        row = kept_ref[TW * y : TW * (y + 1)]
        head = left_ref[EW * y : EW * (y + 1)]
        if y < EH:
            row = row + upper_ref[TW * y : TW * (y + 1)]
            head = head + corner_ref[EW * y : EW * (y + 1)]
        row = jnp.concatenate([row[:EW] + head, row[EW:]], axis=0)
        ratio = row[:, :P_SIZE] / row[:, P_SIZE:]
        for x in range(TW):
            out_ref[y : y + 1, P_SIZE * x : P_SIZE * (x + 1)] = ratio[x : x + 1]


VM = pl.BlockSpec(memory_space=pltpu.VMEM)
SM = pl.BlockSpec(memory_space=pltpu.SMEM)


def call(kernel, outs, scratch=(), smem=0, limit=None):
    def run(*args):
        return pl.pallas_call(
            kernel,
            out_shape=[jax.ShapeDtypeStruct(s, d) for s, d in outs],
            in_specs=[SM] * smem + [VM] * (len(args) - smem),
            out_specs=[VM] * len(outs),
            scratch_shapes=[pltpu.VMEM(s, d) for s, d in scratch],
            compiler_params=pltpu.CompilerParams(vmem_limit_bytes=limit),
        )(*args)

    return run


MB = 1 << 20


def shards(
    latent,
    attn_shift,
    attn_scale,
    attn_gate,
    final_shift,
    final_scale,
    q_weight,
    k_weight,
    v_weight,
    o_weight,
    out_weight,
    neighbour_mask,
    blend_weight,
):
    shift, scale, gate = (v.reshape(1, D) for v in (attn_shift, attn_scale, attn_gate))
    fshift, fscale = (v.reshape(1, D) for v in (final_shift, final_scale))
    mask = neighbour_mask.reshape(4)
    halo = call(
        pack_kernel,
        [((TH * EW, D), BF16), ((EH * TW, D), BF16), ((EH * EW, D), BF16)],
        limit=4 * MB,
    )(latent)
    right, lower, corner = fetch(halo[0], 0, 1), fetch(halo[1], 1, 0), fetch(halo[2], 1, 1)
    win, to_up, to_down, to_left, to_right = call(
        assemble_kernel, [((OWN, D), BF16)] + [((SIDE, D), BF16)] * 4, limit=8 * MB
    )(latent, right, lower, corner)
    from_left, from_right = fetch(to_right, 0, -1), fetch(to_left, 0, 1)
    from_up, from_down = fetch(to_down, -1, 0), fetch(to_up, 1, 0)
    q, k, v = call(own_kernel, [((OWN, AD), BF16)] * 3, limit=24 * MB)(
        win, scale, shift, q_weight, k_weight, v_weight
    )
    kept, spill_e, spill_s, spill_c = call(
        rest_kernel,
        [
            ((TH * TW, LANES), F32),
            ((TH * EW, LANES), F32),
            ((EH * TW, LANES), F32),
            ((EH * EW, LANES), F32),
        ],
        scratch=[
            ((KEYS - OWN, D), BF16),
            ((KEYS, AD), BF16),
            ((PAIRS, KEYS, 2 * LANES), BF16),
            ((OWN, AD), BF16),
        ],
        smem=1,
        limit=32 * MB,
    )(
        mask, win, q, k, v, from_up, from_down, from_left, from_right,
        scale, shift, gate, fscale, fshift, k_weight, v_weight, o_weight, out_weight, blend_weight,
    )
    left, upper, diag = fetch(spill_e, 0, -1), fetch(spill_s, -1, 0), fetch(spill_c, -1, -1)
    (out,) = call(blend_kernel, [((TH, TW * P_SIZE), F32)], limit=4 * MB)(kept, left, upper, diag)
    return out


def solution(mesh):
    in_specs = (
        P("row", "col", None),
        P(),
        P(),
        P(),
        P(),
        P(),
        P(),
        P(),
        P(),
        P(),
        P(),
        P("row", "col", None),
        P("row", "col"),
    )
    out_specs = P("row", "col")
    return jax.shard_map(shards, mesh=mesh, in_specs=in_specs, out_specs=out_specs, check_vma=False)
```

```python
import jax
import jax.numpy as jnp
from jax import lax
from jax.experimental import pallas as pl
from jax.experimental.pallas import tpu as pltpu
from jax.sharding import PartitionSpec as P


D = 1536
HD = 64
HEADS = 12
P_SIZE = 64
TH = 6
TW = 12
EH = 2
EW = 4
WH = 8
WW = 16
AD = HEADS * HD
PAIRS = HEADS // 2
OWN = WH * WW
SIDE = TH * WW
MID = TW - EW
EARLY = 4 * 128
LATE = 128
PARTS = 4
LANES = 128

EPSILON = 1e-06
BLOCKED = -1e30
F32 = jnp.float32
BF16 = jnp.bfloat16


def fetch(block, down, right):
    n_row, n_col = lax.axis_size("row"), lax.axis_size("col")
    route = [
        (((r + down) % n_row) * n_col + (c + right) % n_col, r * n_col + c)
        for r in range(n_row)
        for c in range(n_col)
    ]
    return lax.ppermute(block, ("row", "col"), route)


def layer_norm(features, scale, shift):
    center = features - jnp.mean(features, axis=-1, keepdims=True)
    spread = jnp.mean(center * center, axis=-1, keepdims=True)
    normed = center * lax.rsqrt(spread + EPSILON)
    return (normed * (1.0 + scale) + shift).astype(BF16)


def dot(a, b):
    return jnp.dot(a, b, preferred_element_type=F32)


def pack_kernel(x_ref, right_ref, lower_ref, corner_ref, tile_ref, mid_ref):
    for r in range(TH):
        row = x_ref[r]
        right_ref[EW * r : EW * (r + 1)] = row[:EW]
        tile_ref[TW * r : TW * (r + 1)] = row
        mid_ref[MID * r : MID * (r + 1)] = row[EW:]
        if r < EH:
            lower_ref[TW * r : TW * (r + 1)] = row
            corner_ref[EW * r : EW * (r + 1)] = row[:EW]


def load_kernel(*refs):
    count = len(refs) - 1
    sources, targets, sems = refs[: count // 2], refs[count // 2 : count], refs[count]
    copies = []
    for i, (source, target) in enumerate(zip(sources, targets)):
        rows = source.shape[0] // PARTS
        for k in range(PARTS):
            at = pl.ds(rows * k, rows)
            copies.append(pltpu.make_async_copy(source.at[at], target.at[at], sems.at[i, k]))
    for copy in copies:
        copy.start()
    for copy in copies:
        copy.wait()


def assemble_kernel(tile_ref, right_ref, lower_ref, corner_ref, win_ref, up_ref, down_ref, late_ref):
    for r in range(WH):
        k = r - TH
        if r < TH:
            body, tail = tile_ref[TW * r : TW * (r + 1)], right_ref[EW * r : EW * (r + 1)]
        else:
            body, tail = lower_ref[TW * k : TW * (k + 1)], corner_ref[EW * k : EW * (k + 1)]
            late_ref[EW * WH + MID * k : EW * WH + MID * (k + 1)] = body[EW:]
        late_ref[EW * r : EW * (r + 1)] = tail
        row = jnp.concatenate([body, tail], axis=0)
        win_ref[WW * r : WW * (r + 1)] = row
        if r >= EH:
            up_ref[WW * (r - EH) : WW * (r - EH + 1)] = row
        if r < TH:
            down_ref[WW * r : WW * (r + 1)] = row


def own_kernel(win_ref, scale_ref, shift_ref, qw_ref, kw_ref, vw_ref, q_ref, k_ref, v_ref):
    normed = layer_norm(win_ref[...].astype(F32), vec(scale_ref), vec(shift_ref))
    q_ref[...] = (dot(normed, qw_ref[...]).astype(BF16)) * BF16(HD**-0.5)
    k_ref[...] = dot(normed, kw_ref[...]).astype(BF16)
    v_ref[...] = dot(normed, vw_ref[...]).astype(BF16)


def vec(ref):
    return ref[...].reshape(1, D)


def two_heads(q_ref, p):
    lane = lax.broadcasted_iota(jnp.int32, (OWN, LANES), 1)
    q = q_ref[:, LANES * p : LANES * (p + 1)]
    zero = jnp.zeros_like(q)
    return jnp.concatenate([jnp.where(lane < HD, q, zero), jnp.where(lane < HD, zero, q)], axis=0)


def scores_of(q, keys):
    return lax.dot_general(q, keys, (((1,), (1,)), ((), ())), preferred_element_type=F32)


def shut_row(count, spans):
    place = lax.broadcasted_iota(jnp.int32, (1, count), 1)
    shut = jnp.full((1, count), BLOCKED, F32)
    for start, stop, live in spans:
        inside = (place >= start) & (place < stop) & (live > 0)
        shut = jnp.where(inside, 0.0, shut)
    return shut


def mid_kernel(
    mask_ref, q_ref, k_ref, v_ref, up_ref, down_ref, left_ref, right_ref,
    scale_ref, shift_ref, kw_ref, vw_ref,
    state_ref, top_ref,
    normed_ref, keys_ref, vals_ref,
):
    scale, shift = vec(scale_ref), vec(shift_ref)
    spans, at = [], 0
    for j, side in enumerate((up_ref, down_ref, left_ref, right_ref)):
        size = side.shape[0]
        normed_ref[at : at + size] = layer_norm(side[...].astype(F32), scale, shift)
        spans.append((OWN + at, OWN + at + size, mask_ref[j]))
        at += size
    normed_ref[at:] = jnp.zeros((EARLY - OWN - at, D), BF16)
    normed = normed_ref[...]
    keys_ref[:OWN] = k_ref[...]
    keys_ref[OWN:] = dot(normed, kw_ref[...]).astype(BF16)
    values = dot(normed, vw_ref[...]).astype(BF16)
    for p in range(PAIRS):
        vals_ref[p, :OWN, :LANES] = v_ref[:, LANES * p : LANES * (p + 1)]
        vals_ref[p, OWN:, :LANES] = values[:, LANES * p : LANES * (p + 1)]
        vals_ref[p, :, LANES:] = jnp.ones((EARLY, LANES), BF16)
    token = lax.broadcasted_iota(jnp.int32, (1, OWN), 1)
    row, col = token // WW, token % WW
    times = 1 + jnp.where(row < EH, mask_ref[0], 0) + jnp.where(row >= TH, mask_ref[1], 0)
    times = times + jnp.where(col < EW, mask_ref[2], 0) + jnp.where(col >= TW, mask_ref[3], 0)
    times = jnp.concatenate([times.astype(F32), jnp.ones((1, EARLY - OWN), F32)], axis=1)
    shut = shut_row(EARLY, [(0, OWN, 1)] + spans)
    for p in range(PAIRS):
        scores = scores_of(two_heads(q_ref, p), keys_ref[:, LANES * p : LANES * (p + 1)]) + shut
        top = jnp.max(scores, axis=-1, keepdims=True)
        weights = (jnp.exp(scores - top) * times).astype(BF16)
        state_ref[p] = dot(weights, vals_ref[p])
        top_ref[p] = jnp.broadcast_to(top, (2 * OWN, LANES))


def last_kernel(
    mask_ref, win_ref, q_ref, left_ref, right_ref, state_ref, top_ref,
    scale_ref, shift_ref, gate_ref, fscale_ref, fshift_ref,
    kw_ref, vw_ref, ow_ref, pw_ref, blend_ref,
    kept_ref, spill_e_ref, spill_s_ref, spill_c_ref,
    normed_ref, vals_ref, att_ref,
):
    scale, shift = vec(scale_ref), vec(shift_ref)
    one, two = left_ref.shape[0], left_ref.shape[0] + right_ref.shape[0]
    normed_ref[:one] = layer_norm(left_ref[...].astype(F32), scale, shift)
    normed_ref[one:two] = layer_norm(right_ref[...].astype(F32), scale, shift)
    normed_ref[two:] = jnp.zeros((LATE - two, D), BF16)
    normed = normed_ref[...]
    keys = dot(normed, kw_ref[...]).astype(BF16)
    values = dot(normed, vw_ref[...]).astype(BF16)
    shut = shut_row(LATE, [(0, one, mask_ref[2]), (one, two, mask_ref[3])])
    first = lax.broadcasted_iota(jnp.int32, (OWN, LANES), 1) < HD
    for p in range(PAIRS):
        vals_ref[:, :LANES] = values[:, LANES * p : LANES * (p + 1)]
        vals_ref[:, LANES:] = jnp.ones((LATE, LANES), BF16)
        scores = scores_of(two_heads(q_ref, p), keys[:, LANES * p : LANES * (p + 1)]) + shut
        before = top_ref[p]
        top = jnp.maximum(before, jnp.max(scores, axis=-1, keepdims=True))
        weights = jnp.exp(scores - top).astype(BF16)
        fade = jnp.exp(before - top)
        new = dot(weights, vals_ref[...])
        out = state_ref[p, :, :LANES] * fade + new[:, :LANES]
        out = out / (state_ref[p, :, LANES:] * fade + new[:, LANES:])
        att_ref[:, LANES * p : LANES * (p + 1)] = jnp.where(first, out[:OWN], out[OWN:]).astype(BF16)

    mixed = win_ref[...].astype(F32) + vec(gate_ref) * dot(att_ref[...], ow_ref[...])
    final = layer_norm(mixed, vec(fscale_ref), vec(fshift_ref))
    patch = scores_of(final, pw_ref[...])
    spread = jnp.concatenate(
        [jnp.broadcast_to(blend_ref[r : r + 1], (WW, WW)) for r in range(WH)], axis=0
    )
    own_row = lax.broadcasted_iota(jnp.int32, (OWN, WW), 0) % WW
    own_col = lax.broadcasted_iota(jnp.int32, (OWN, WW), 1)
    b = jnp.sum(jnp.where(own_row == own_col, spread, 0.0), axis=1, keepdims=True)
    both = jnp.concatenate([b * patch, jnp.broadcast_to(b, (OWN, P_SIZE))], axis=1)
    for r in range(WH):
        at = WW * r
        if r < TH:
            kept_ref[TW * r : TW * (r + 1)] = both[at : at + TW]
            spill_e_ref[EW * r : EW * (r + 1)] = both[at + TW : at + WW]
        else:
            k = r - TH
            spill_s_ref[TW * k : TW * (k + 1)] = both[at : at + TW]
            spill_c_ref[EW * k : EW * (k + 1)] = both[at + TW : at + WW]


def blend_kernel(kept_ref, left_ref, upper_ref, corner_ref, out_ref):
    for y in range(TH):
        row = kept_ref[TW * y : TW * (y + 1)]
        head = left_ref[EW * y : EW * (y + 1)]
        if y < EH:
            row = row + upper_ref[TW * y : TW * (y + 1)]
            head = head + corner_ref[EW * y : EW * (y + 1)]
        row = jnp.concatenate([row[:EW] + head, row[EW:]], axis=0)
        ratio = row[:, :P_SIZE] / row[:, P_SIZE:]
        for x in range(TW):
            out_ref[y : y + 1, P_SIZE * x : P_SIZE * (x + 1)] = ratio[x : x + 1]


VM = pl.BlockSpec(memory_space=pltpu.VMEM)
SM = pl.BlockSpec(memory_space=pltpu.SMEM)
HB = pl.BlockSpec(memory_space=pltpu.HBM)
MB = 1 << 20


def call(kernel, outs, scratch=(), smem=0, limit=None, ins=VM):
    def launch(*args):
        return pl.pallas_call(
            kernel,
            out_shape=[jax.ShapeDtypeStruct(s, d) for s, d in outs],
            in_specs=[SM] * smem + [ins] * (len(args) - smem),
            out_specs=[VM] * len(outs),
            scratch_shapes=list(scratch),
            compiler_params=pltpu.CompilerParams(vmem_limit_bytes=limit),
        )(*args)

    return launch


def block(
    latent, attn_shift, attn_scale, attn_gate, final_shift, final_scale,
    q_weight, k_weight, v_weight, o_weight, out_weight, neighbour_mask, blend_weight,
):
    mask = neighbour_mask.reshape(4)
    right, lower, corner, tile, mid = call(
        pack_kernel,
        [(n, BF16) for n in ((TH * EW, D), (EH * TW, D), (EH * EW, D), (TH * TW, D), (TH * MID, D))],
        limit=4 * MB,
    )(latent)
    right = fetch(right, 0, 1)
    corner = fetch(corner, 1, 1)
    lower = fetch(lower, 1, 0)
    left_early, right_early = fetch(tile, 0, -1), fetch(mid, 0, 1)
    weights = (q_weight, k_weight, v_weight, o_weight)
    qw, kw, vw, ow = call(
        load_kernel,
        [(w.shape, BF16) for w in weights],
        scratch=[pltpu.SemaphoreType.DMA((len(weights), PARTS))],
        limit=MB,
        ins=HB,
    )(*(pltpu.with_memory_space_constraint(w, pltpu.HBM) for w in weights))
    win, to_up, to_down, late = call(
        assemble_kernel,
        [(n, BF16) for n in ((OWN, D), (SIDE, D), (SIDE, D), (WH * EW + EH * MID, D))],
        limit=8 * MB,
    )(tile, right, lower, corner)
    left_late, right_late = fetch(lower, 0, -1), fetch(late, 0, 1)
    from_up, from_down = fetch(to_down, -1, 0), fetch(to_up, 1, 0)
    q, k, v = call(own_kernel, [((OWN, AD), BF16)] * 3, limit=12 * MB)(
        win, attn_scale, attn_shift, qw, kw, vw
    )
    state, top = call(
        mid_kernel,
        [((PAIRS, 2 * OWN, 2 * LANES), F32), ((PAIRS, 2 * OWN, LANES), F32)],
        scratch=[
            pltpu.VMEM((EARLY - OWN, D), BF16),
            pltpu.VMEM((EARLY, AD), BF16),
            pltpu.VMEM((PAIRS, EARLY, 2 * LANES), BF16),
        ],
        smem=1,
        limit=20 * MB,
    )(mask, q, k, v, from_up, from_down, left_early, right_early, attn_scale, attn_shift, kw, vw)
    kept, spill_e, spill_s, spill_c = call(
        last_kernel,
        [(n, F32) for n in ((TH * TW, LANES), (TH * EW, LANES), (EH * TW, LANES), (EH * EW, LANES))],
        scratch=[
            pltpu.VMEM((LATE, D), BF16),
            pltpu.VMEM((LATE, 2 * LANES), BF16),
            pltpu.VMEM((OWN, AD), BF16),
        ],
        smem=1,
        limit=16 * MB,
    )(
        mask, win, q, left_late, right_late, state, top,
        attn_scale, attn_shift, attn_gate, final_scale, final_shift,
        kw, vw, ow, out_weight.T, blend_weight,
    )
    left = fetch(spill_e, 0, -1)
    diag = fetch(spill_c, -1, -1)
    upper = fetch(spill_s, -1, 0)
    (out,) = call(blend_kernel, [((TH, TW * P_SIZE), F32)], limit=4 * MB)(kept, left, upper, diag)
    return out


def solution(mesh):
    in_specs = (
        P("row", "col", None),
        P(),
        P(),
        P(),
        P(),
        P(),
        P(),
        P(),
        P(),
        P(),
        P(),
        P("row", "col", None),
        P("row", "col"),
    )
    out_specs = P("row", "col")
    return jax.shard_map(block, mesh=mesh, in_specs=in_specs, out_specs=out_specs, check_vma=False)
```

```python
import jax
import jax.numpy as jnp
import numpy as np
from jax import lax
from jax.experimental import pallas as pl
from jax.experimental.pallas import tpu as pltpu
from jax.sharding import PartitionSpec as P


D = 1536
HD = 64
HEADS = 12
P_SIZE = 64
TH = 6
TW = 12
EH = 2
EW = 4
WH = 8
WW = 16
AD = HEADS * HD
PAIRS = HEADS // 2
LANES = 128
OWN = WH * WW
TILE = TH * TW
SIDE = TH * EW
TOP = EH * TW
CORNER = EH * EW
REST = TILE - TOP
RELAY = SIDE + EH * (TW - EW) + CORNER + TOP
EARLY = TILE + 2 * TILE + SIDE + TILE + TOP + TOP
LATE = RELAY + SIDE + REST + CORNER
KEYS = EARLY + LATE

EPSILON = 1e-06
BLOCKED = -1e30
F32 = jnp.float32
BF16 = jnp.bfloat16
MB = 1 << 20


def grid(rows, cols):
    return [(r, c) for r in rows for c in cols]


def places():
    tile_r, top_r, rest_r = range(TH), range(EH), range(EH, TH)
    tile_c, edge_c, body_c = range(TW), range(EW), range(EW, TW)

    def shift(cells, down, right):
        return [(r + down, c + right) for r, c in cells]

    tile, top = grid(tile_r, tile_c), grid(top_r, tile_c)
    packed = grid(tile_r, edge_c) + grid(tile_r, body_c)
    side, corner = grid(tile_r, edge_c), grid(top_r, edge_c)
    relay = shift(packed[: SIDE + EH * (TW - EW)], 0, TW) + shift(corner, 0, 2 * TW) + shift(top, 0, -TW)
    return (
        tile
        + shift(packed, 0, TW)
        + shift(tile, TH, 0)
        + shift(side, 0, 2 * TW)
        + shift(tile, -TH, 0)
        + shift(top, 2 * TH, 0)
        + shift(top, 0, -TW)
        + shift(relay, TH, 0)
        + shift(side, -TH, TW)
        + shift(grid(rest_r, tile_c), 0, -TW)
        + shift(corner, 2 * TH, TW)
    )


def coverage():
    table = np.zeros((8, KEYS), np.float32)
    cells = places()
    assert len(set(cells)) == len(cells) == KEYS
    for j, (down, right) in enumerate(((0, 0), (-TH, 0), (TH, 0), (0, -TW), (0, TW))):
        for k, (r, c) in enumerate(cells):
            table[j, k] = 0 <= r - down < WH and 0 <= c - right < WW
    assert table.sum() == 5 * OWN
    return table


def query_columns():
    cells = grid(range(TH), range(TW)) + grid(range(TH), range(TW, WW))
    cells += grid(range(TH, WH), range(TW)) + grid(range(TH, WH), range(TW, WW))
    return np.eye(WW, dtype=np.float32)[[c for _, c in cells]]


def fetch(block, down, right):
    n_row, n_col = lax.axis_size("row"), lax.axis_size("col")
    route = [
        (((r + down) % n_row) * n_col + (c + right) % n_col, r * n_col + c)
        for r in range(n_row)
        for c in range(n_col)
    ]
    return lax.ppermute(block, ("row", "col"), route)


def vec(ref):
    return ref[...].reshape(1, D)


def layer_norm(features, scale, shift):
    center = features - jnp.mean(features, axis=-1, keepdims=True)
    spread = jnp.mean(center * center, axis=-1, keepdims=True)
    normed = center * lax.rsqrt(spread + EPSILON)
    return (normed * (1.0 + scale) + shift).astype(BF16)


def dot(a, b):
    return jnp.dot(a, b, preferred_element_type=F32)


def dot_t(a, b):
    return lax.dot_general(a, b, (((1,), (1,)), ((), ())), preferred_element_type=F32)


def query(normed, qw_ref):
    return dot(normed, qw_ref[...]).astype(BF16) * BF16(HD**-0.5)


def pack_kernel(x_ref, tile_ref, top_ref, rest_ref, packed_ref, side_ref):
    mid = TW - EW
    for r in range(TH):
        row = x_ref[r]
        tile_ref[TW * r : TW * (r + 1)] = row
        if r < EH:
            top_ref[TW * r : TW * (r + 1)] = row
        else:
            rest_ref[TW * (r - EH) : TW * (r - EH + 1)] = row
        side_ref[EW * r : EW * (r + 1)] = row[:EW]
        packed_ref[EW * r : EW * (r + 1)] = row[:EW]
        packed_ref[SIDE + mid * r : SIDE + mid * (r + 1)] = row[EW:]


def relay_kernel(east_ref, far_ref, top_ref, up_ref, down_ref, twice_ref):
    cut = SIDE + EH * (TW - EW)
    up_ref[:cut] = east_ref[:cut]
    up_ref[cut : cut + CORNER] = far_ref[:CORNER]
    up_ref[cut + CORNER :] = top_ref[...]
    down_ref[...] = east_ref[:SIDE]
    twice_ref[...] = east_ref[:CORNER]


def own_kernel(tile_ref, scale_ref, shift_ref, qw_ref, kw_ref, vw_ref, q_ref, k_ref, v_ref):
    normed = layer_norm(tile_ref[...].astype(F32), vec(scale_ref), vec(shift_ref))
    q_ref[...] = query(normed, qw_ref)
    k_ref[...] = dot(normed, kw_ref[...]).astype(BF16)
    v_ref[...] = dot(normed, vw_ref[...]).astype(BF16)


def norm_blocks(blocks, normed_ref, scale, shift):
    at = 0
    for block in blocks:
        size = block.shape[0]
        normed_ref[at : at + size] = layer_norm(block[...].astype(F32), scale, shift)
        at += size


def mid_kernel(
    east_ref, south_ref, far_ref, north_ref, low_ref, west_ref,
    scale_ref, shift_ref, qw_ref, kw_ref, vw_ref,
    q_ref, k_ref, v_ref,
    normed_ref,
):
    blocks = (east_ref, south_ref, far_ref, north_ref, low_ref, west_ref)
    norm_blocks(blocks, normed_ref, vec(scale_ref), vec(shift_ref))
    normed = normed_ref[...]
    k_ref[...] = dot(normed, kw_ref[...]).astype(BF16)
    v_ref[...] = dot(normed, vw_ref[...]).astype(BF16)
    halo = jnp.concatenate([normed_ref[:SIDE], normed_ref[TILE : TILE + TOP]], axis=0)
    q_ref[...] = query(halo, qw_ref)


def last_kernel(
    mask_ref, cover_ref, pick_ref, tile_ref, east_ref, south_ref,
    relay_ref, side_ref, rest_ref, corner_ref,
    q0_ref, k0_ref, v0_ref, q1_ref, k1_ref, v1_ref,
    scale_ref, shift_ref, gate_ref, fscale_ref, fshift_ref,
    qw_ref, kw_ref, vw_ref, ow_ref, pw_ref, blend_ref,
    kept_ref, spill_e_ref, spill_s_ref, spill_c_ref,
    normed_ref, queries_ref, keys_ref, vals_ref, att_ref,
):
    norm_blocks((relay_ref, side_ref, rest_ref, corner_ref), normed_ref, vec(scale_ref), vec(shift_ref))
    normed = normed_ref[...]
    queries_ref[:TILE] = q0_ref[...]
    queries_ref[TILE : OWN - CORNER] = q1_ref[...]
    queries_ref[OWN - CORNER :] = query(normed_ref[: 2 * CORNER], qw_ref)[:CORNER]
    keys_ref[:TILE] = k0_ref[...]
    keys_ref[TILE:EARLY] = k1_ref[...]
    keys_ref[EARLY:] = dot(normed, kw_ref[...]).astype(BF16)
    values = dot(normed, vw_ref[...]).astype(BF16)

    times = cover_ref[0:1]
    for j in range(4):
        times = times + cover_ref[j + 1 : j + 2] * (mask_ref[j] > 0).astype(F32)
    shut = jnp.where(times > 0, 0.0, BLOCKED)
    lane = lax.broadcasted_iota(jnp.int32, (OWN, LANES), 1)
    for p in range(PAIRS):
        at = slice(LANES * p, LANES * (p + 1))
        vals_ref[:TILE, :LANES] = v0_ref[:, at]
        vals_ref[TILE:EARLY, :LANES] = v1_ref[:, at]
        vals_ref[EARLY:, :LANES] = values[:, at]
        if p == 0:
            vals_ref[:, LANES:] = jnp.ones((KEYS, LANES), BF16)
        q = queries_ref[:, at]
        zero = jnp.zeros_like(q)
        both = jnp.concatenate([jnp.where(lane < HD, q, zero), jnp.where(lane < HD, zero, q)], axis=0)
        scores = dot_t(both, keys_ref[:, at]) + shut
        top = jnp.max(scores, axis=-1, keepdims=True)
        weights = (jnp.exp(scores - top) * times).astype(BF16)
        out = dot(weights, vals_ref[...])
        out = out[:, :LANES] / out[:, LANES:]
        att_ref[:, at] = jnp.where(lane < HD, out[:OWN], out[OWN:]).astype(BF16)

    window = jnp.concatenate(
        [tile_ref[...], east_ref[:SIDE], south_ref[:TOP], relay_ref[:CORNER]], axis=0
    )
    mixed = window.astype(F32) + vec(gate_ref) * dot(att_ref[...], ow_ref[...])
    final = layer_norm(mixed, vec(fscale_ref), vec(fshift_ref))
    patch = dot_t(final, pw_ref[...])
    spans = [(r, TW) for r in range(TH)] + [(r, EW) for r in range(TH)]
    spans += [(r, TW) for r in range(TH, WH)] + [(r, EW) for r in range(TH, WH)]
    spread = jnp.concatenate(
        [jnp.broadcast_to(blend_ref[r : r + 1], (n, WW)) for r, n in spans], axis=0
    )
    b = jnp.sum(spread * pick_ref[...], axis=1, keepdims=True)
    both = jnp.concatenate([b * patch, jnp.broadcast_to(b, (OWN, P_SIZE))], axis=1)
    kept_ref[...] = both[:TILE]
    spill_e_ref[...] = both[TILE : TILE + SIDE]
    spill_s_ref[...] = both[TILE + SIDE : OWN - CORNER]
    spill_c_ref[...] = both[OWN - CORNER :]


def blend_kernel(kept_ref, left_ref, upper_ref, corner_ref, out_ref):
    for y in range(TH):
        row = kept_ref[TW * y : TW * (y + 1)]
        head = left_ref[EW * y : EW * (y + 1)]
        if y < EH:
            row = row + upper_ref[TW * y : TW * (y + 1)]
            head = head + corner_ref[EW * y : EW * (y + 1)]
        row = jnp.concatenate([row[:EW] + head, row[EW:]], axis=0)
        ratio = row[:, :P_SIZE] / row[:, P_SIZE:]
        for x in range(TW):
            out_ref[y : y + 1, P_SIZE * x : P_SIZE * (x + 1)] = ratio[x : x + 1]


VM = pl.BlockSpec(memory_space=pltpu.VMEM)
SM = pl.BlockSpec(memory_space=pltpu.SMEM)


def call(kernel, outs, *args, scratch=(), smem=0, limit=None, flops=0):
    cost = pl.CostEstimate(flops=flops, bytes_accessed=0, transcendentals=0) if flops else None
    return pl.pallas_call(
        kernel,
        out_shape=[jax.ShapeDtypeStruct(s, d) for s, d in outs],
        in_specs=[SM] * smem + [VM] * (len(args) - smem),
        out_specs=[VM] * len(outs),
        scratch_shapes=[pltpu.VMEM(s, d) for s, d in scratch],
        compiler_params=pltpu.CompilerParams(vmem_limit_bytes=limit),
        cost_estimate=cost,
    )(*args)


def block(
    latent,
    attn_shift,
    attn_scale,
    attn_gate,
    final_shift,
    final_scale,
    q_weight,
    k_weight,
    v_weight,
    o_weight,
    out_weight,
    neighbour_mask,
    blend_weight,
):
    mask = neighbour_mask.reshape(4)
    tile, top, rest, packed, side = call(
        pack_kernel,
        [((n, D), BF16) for n in (TILE, TOP, REST, TILE, SIDE)],
        latent,
        limit=4 * MB,
        flops=1 << 33,
    )
    east, far = fetch(packed, 0, 1), fetch(side, 0, 2)
    west_top, west_rest = fetch(top, 0, -1), fetch(rest, 0, -1)
    north, south = fetch(tile, -1, 0), fetch(tile, 1, 0)
    low = fetch(top, 2, 0)
    q0, k0, v0 = call(
        own_kernel,
        [((TILE, AD), BF16)] * 3,
        tile, attn_scale, attn_shift, q_weight, k_weight, v_weight,
        limit=8 * MB,
    )
    to_up, to_down, to_twice = call(
        relay_kernel,
        [((n, D), BF16) for n in (RELAY, SIDE, CORNER)],
        east, far, west_top,
        limit=4 * MB,
    )
    relayed = fetch(to_up, 1, 0)
    north_side = fetch(to_down, -1, 0)
    low_corner = fetch(to_twice, 2, 0)
    q1, k1, v1 = call(
        mid_kernel,
        [((n, AD), BF16) for n in (SIDE + TOP, EARLY - TILE, EARLY - TILE)],
        east, south, far, north, low, west_top,
        attn_scale, attn_shift, q_weight, k_weight, v_weight,
        scratch=[((EARLY - TILE, D), BF16)],
        limit=12 * MB,
    )
    kept, spill_e, spill_s, spill_c = call(
        last_kernel,
        [((n, LANES), F32) for n in (TILE, SIDE, TOP, CORNER)],
        mask, jnp.asarray(coverage()), jnp.asarray(query_columns()), tile, east, south,
        relayed, north_side, west_rest, low_corner,
        q0, k0, v0, q1, k1, v1,
        attn_scale, attn_shift, attn_gate, final_scale, final_shift,
        q_weight, k_weight, v_weight, o_weight, out_weight.T, blend_weight,
        scratch=[
            ((LATE, D), BF16),
            ((OWN, AD), BF16),
            ((KEYS, AD), BF16),
            ((KEYS, 2 * LANES), BF16),
            ((OWN, AD), BF16),
        ],
        smem=1,
        limit=20 * MB,
    )
    left = fetch(spill_e, 0, -1)
    diag = fetch(spill_c, -1, -1)
    upper = fetch(spill_s, -1, 0)
    (out,) = call(blend_kernel, [((TH, TW * P_SIZE), F32)], kept, left, upper, diag, limit=4 * MB)
    return out


def solution(mesh):
    in_specs = (
        P("row", "col", None),
        P(),
        P(),
        P(),
        P(),
        P(),
        P(),
        P(),
        P(),
        P(),
        P(),
        P("row", "col", None),
        P("row", "col"),
    )
    out_specs = P("row", "col")
    return jax.shard_map(block, mesh=mesh, in_specs=in_specs, out_specs=out_specs, check_vma=False)
```

```python
import jax
import jax.numpy as jnp
import numpy as np
from jax import lax
from jax.experimental import pallas as pl
from jax.experimental.pallas import tpu as pltpu
from jax.sharding import PartitionSpec as P


D = 1536
HD = 64
HEADS = 12
P_SIZE = 64
TH = 6
TW = 12
EH = 2
EW = 4
WH = 8
WW = 16
AD = HEADS * HD
PAIRS = HEADS // 2
LANES = 128
OWN = WH * WW
TILE = TH * TW
SIDE = TH * EW
TOP = EH * TW
CORNER = EH * EW
REST = TILE - TOP
RELAY = SIDE + EH * (TW - EW) + CORNER + TOP
CUT = SIDE + EH * (TW - EW)
EARLY = TILE + 2 * TILE + SIDE + TILE + TOP + TOP
LATE = RELAY + SIDE + REST + CORNER
KEYS = EARLY + LATE

EPSILON = 1e-06
BLOCKED = -1e30
F32 = jnp.float32
BF16 = jnp.bfloat16
MB = 1 << 20


def grid(rows, cols):
    return [(r, c) for r in rows for c in cols]


def places():
    tile_r, top_r, rest_r = range(TH), range(EH), range(EH, TH)
    tile_c, edge_c, body_c = range(TW), range(EW), range(EW, TW)

    def shift(cells, down, right):
        return [(r + down, c + right) for r, c in cells]

    tile, top = grid(tile_r, tile_c), grid(top_r, tile_c)
    packed = grid(tile_r, edge_c) + grid(tile_r, body_c)
    side, corner = grid(tile_r, edge_c), grid(top_r, edge_c)
    relay = shift(packed[:CUT], 0, TW) + shift(corner, 0, 2 * TW) + shift(top, 0, -TW)
    return (
        tile
        + shift(packed[:CUT], 0, TW)
        + shift(tile, TH, 0)
        + shift(side, 0, 2 * TW)
        + shift(tile, -TH, 0)
        + shift(top, 2 * TH, 0)
        + shift(top, 0, -TW)
        + shift(packed[CUT:], 0, TW)
        + shift(relay, TH, 0)
        + shift(side, -TH, TW)
        + shift(grid(rest_r, tile_c), 0, -TW)
        + shift(corner, 2 * TH, TW)
    )


def coverage():
    table = np.zeros((8, KEYS), np.float32)
    cells = places()
    assert len(set(cells)) == len(cells) == KEYS
    for j, (down, right) in enumerate(((0, 0), (-TH, 0), (TH, 0), (0, -TW), (0, TW))):
        for k, (r, c) in enumerate(cells):
            table[j, k] = 0 <= r - down < WH and 0 <= c - right < WW
    assert table.sum() == 5 * OWN
    return table


def query_columns():
    cells = grid(range(TH), range(TW)) + grid(range(TH), range(TW, WW))
    cells += grid(range(TH, WH), range(TW)) + grid(range(TH, WH), range(TW, WW))
    return np.eye(WW, dtype=np.float32)[[c for _, c in cells]]


def fetch(block, down, right):
    n_row, n_col = lax.axis_size("row"), lax.axis_size("col")
    route = [
        (((r + down) % n_row) * n_col + (c + right) % n_col, r * n_col + c)
        for r in range(n_row)
        for c in range(n_col)
    ]
    return lax.ppermute(block, ("row", "col"), route)


def vec(ref):
    return ref[...].reshape(1, D)


def layer_norm(features, scale, shift):
    center = features - jnp.mean(features, axis=-1, keepdims=True)
    spread = jnp.mean(center * center, axis=-1, keepdims=True)
    normed = center * lax.rsqrt(spread + EPSILON)
    return (normed * (1.0 + scale) + shift).astype(BF16)


def dot(a, b):
    return jnp.dot(a, b, preferred_element_type=F32)


def dot_t(a, b):
    return lax.dot_general(a, b, (((1,), (1,)), ((), ())), preferred_element_type=F32)


def query(normed, qw_ref):
    return dot(normed, qw_ref[...]).astype(BF16) * BF16(HD**-0.5)


def pack_kernel(x_ref, tile_ref, top_ref, rest_ref, near_ref, body_ref, side_ref):
    mid = TW - EW
    for r in range(TH):
        row = x_ref[r]
        tile_ref[TW * r : TW * (r + 1)] = row
        if r < EH:
            top_ref[TW * r : TW * (r + 1)] = row
        else:
            rest_ref[TW * (r - EH) : TW * (r - EH + 1)] = row
        side_ref[EW * r : EW * (r + 1)] = row[:EW]
        near_ref[EW * r : EW * (r + 1)] = row[:EW]
        if r < EH:
            near_ref[SIDE + mid * r : SIDE + mid * (r + 1)] = row[EW:]
        else:
            body_ref[mid * (r - EH) : mid * (r - EH + 1)] = row[EW:]


def relay_kernel(east_ref, far_ref, top_ref, up_ref, down_ref, twice_ref):
    up_ref[:CUT] = east_ref[...]
    up_ref[CUT : CUT + CORNER] = far_ref[:CORNER]
    up_ref[CUT + CORNER :] = top_ref[...]
    down_ref[...] = east_ref[:SIDE]
    twice_ref[...] = east_ref[:CORNER]


def own_kernel(tile_ref, scale_ref, shift_ref, qw_ref, kw_ref, vw_ref, q_ref, k_ref, v_ref):
    normed = layer_norm(tile_ref[...].astype(F32), vec(scale_ref), vec(shift_ref))
    q_ref[...] = query(normed, qw_ref)
    k_ref[...] = dot(normed, kw_ref[...]).astype(BF16)
    v_ref[...] = dot(normed, vw_ref[...]).astype(BF16)


def norm_blocks(blocks, normed_ref, scale, shift):
    at = 0
    for block in blocks:
        size = block.shape[0]
        normed_ref[at : at + size] = layer_norm(block[...].astype(F32), scale, shift)
        at += size


def mid_kernel(
    east_ref, south_ref, far_ref, north_ref, low_ref, west_ref, body_ref,
    scale_ref, shift_ref, qw_ref, kw_ref, vw_ref,
    q_ref, k_ref, v_ref,
    normed_ref,
):
    blocks = (east_ref, south_ref, far_ref, north_ref, low_ref, west_ref, body_ref)
    norm_blocks(blocks, normed_ref, vec(scale_ref), vec(shift_ref))
    normed = normed_ref[...]
    k_ref[...] = dot(normed, kw_ref[...]).astype(BF16)
    v_ref[...] = dot(normed, vw_ref[...]).astype(BF16)
    halo = jnp.concatenate([normed_ref[:SIDE], normed_ref[CUT : CUT + TOP]], axis=0)
    q_ref[...] = query(halo, qw_ref)


def attend(q_ref, k_ref, v_ref, times, att_ref):
    count = q_ref.shape[0]
    shut = jnp.where(times > 0, 0.0, BLOCKED)
    lane = lax.broadcasted_iota(jnp.int32, (count, LANES), 1)
    ones = jnp.ones((KEYS, LANES), BF16)
    for p in range(PAIRS):
        at = slice(LANES * p, LANES * (p + 1))
        q = q_ref[:, at]
        zero = jnp.zeros_like(q)
        both = jnp.concatenate([jnp.where(lane < HD, q, zero), jnp.where(lane < HD, zero, q)], axis=0)
        scores = dot_t(both, k_ref[:, at]) + shut
        top = jnp.max(scores, axis=-1, keepdims=True)
        weights = (jnp.exp(scores - top) * times).astype(BF16)
        out = dot(weights, jnp.concatenate([v_ref[:, at], ones], axis=1))
        out = out[:, :LANES] / out[:, LANES:]
        att_ref[:, at] = jnp.where(lane < HD, out[:count], out[count:]).astype(BF16)


def live_times(mask_ref, cover_ref):
    times = cover_ref[0:1]
    for j in range(4):
        times = times + cover_ref[j + 1 : j + 2] * (mask_ref[j] > 0).astype(F32)
    return times


def finish(tokens, att_ref, gate_ref, fscale_ref, fshift_ref, ow_ref, pw_ref, blend_ref, pick, spans):
    count = tokens.shape[0]
    mixed = tokens.astype(F32) + vec(gate_ref) * dot(att_ref[...], ow_ref[...])
    final = layer_norm(mixed, vec(fscale_ref), vec(fshift_ref))
    patch = dot_t(final, pw_ref[...])
    spread = jnp.concatenate(
        [jnp.broadcast_to(blend_ref[r : r + 1], (n, WW)) for r, n in spans], axis=0
    )
    b = jnp.sum(spread * pick, axis=1, keepdims=True)
    return jnp.concatenate([b * patch, jnp.broadcast_to(b, (count, P_SIZE))], axis=1)


def spill_kernel(
    mask_ref, cover_ref, pick_ref, east_ref, south_ref,
    relay_ref, side_ref, rest_ref, corner_ref,
    k0_ref, v0_ref, q1_ref, k1_ref, v1_ref,
    scale_ref, shift_ref, gate_ref, fscale_ref, fshift_ref,
    qw_ref, kw_ref, vw_ref, ow_ref, pw_ref, blend_ref,
    spill_e_ref, spill_s_ref, spill_c_ref, keys_ref, vals_ref,
    normed_ref, queries_ref, att_ref,
):
    norm_blocks((relay_ref, side_ref, rest_ref, corner_ref), normed_ref, vec(scale_ref), vec(shift_ref))
    normed = normed_ref[...]
    halo = SIDE + TOP
    queries_ref[:halo] = q1_ref[...]
    queries_ref[halo:] = query(normed_ref[: 2 * CORNER], qw_ref)[:CORNER]
    keys_ref[:TILE] = k0_ref[...]
    keys_ref[TILE:EARLY] = k1_ref[...]
    keys_ref[EARLY:] = dot(normed, kw_ref[...]).astype(BF16)
    vals_ref[:TILE] = v0_ref[...]
    vals_ref[TILE:EARLY] = v1_ref[...]
    vals_ref[EARLY:] = dot(normed, vw_ref[...]).astype(BF16)
    attend(queries_ref, keys_ref, vals_ref, live_times(mask_ref, cover_ref), att_ref)
    tokens = jnp.concatenate([east_ref[:SIDE], south_ref[:TOP], relay_ref[:CORNER]], axis=0)
    spans = [(r, EW) for r in range(TH)]
    spans += [(r, TW) for r in range(TH, WH)] + [(r, EW) for r in range(TH, WH)]
    both = finish(
        tokens, att_ref, gate_ref, fscale_ref, fshift_ref, ow_ref, pw_ref, blend_ref,
        pick_ref[TILE:], spans,
    )
    spill_e_ref[...] = both[:SIDE]
    spill_s_ref[...] = both[SIDE:halo]
    spill_c_ref[...] = both[halo:]


def kept_kernel(
    mask_ref, cover_ref, pick_ref, tile_ref, q_ref, keys_ref, vals_ref,
    gate_ref, fscale_ref, fshift_ref, ow_ref, pw_ref, blend_ref,
    kept_ref,
    att_ref,
):
    attend(q_ref, keys_ref, vals_ref, live_times(mask_ref, cover_ref), att_ref)
    kept_ref[...] = finish(
        tile_ref[...], att_ref, gate_ref, fscale_ref, fshift_ref, ow_ref, pw_ref, blend_ref,
        pick_ref[:TILE], [(r, TW) for r in range(TH)],
    )


def blend_kernel(kept_ref, left_ref, upper_ref, corner_ref, out_ref):
    for y in range(TH):
        row = kept_ref[TW * y : TW * (y + 1)]
        head = left_ref[EW * y : EW * (y + 1)]
        if y < EH:
            row = row + upper_ref[TW * y : TW * (y + 1)]
            head = head + corner_ref[EW * y : EW * (y + 1)]
        row = jnp.concatenate([row[:EW] + head, row[EW:]], axis=0)
        ratio = row[:, :P_SIZE] / row[:, P_SIZE:]
        for x in range(TW):
            out_ref[y : y + 1, P_SIZE * x : P_SIZE * (x + 1)] = ratio[x : x + 1]


VM = pl.BlockSpec(memory_space=pltpu.VMEM)
SM = pl.BlockSpec(memory_space=pltpu.SMEM)


def call(kernel, outs, *args, scratch=(), smem=0, limit=None, flops=0):
    cost = pl.CostEstimate(flops=flops, bytes_accessed=0, transcendentals=0) if flops else None
    return pl.pallas_call(
        kernel,
        out_shape=[jax.ShapeDtypeStruct(s, d) for s, d in outs],
        in_specs=[SM] * smem + [VM] * (len(args) - smem),
        out_specs=[VM] * len(outs),
        scratch_shapes=[pltpu.VMEM(s, d) for s, d in scratch],
        compiler_params=pltpu.CompilerParams(vmem_limit_bytes=limit),
        cost_estimate=cost,
    )(*args)


def block(
    latent,
    attn_shift,
    attn_scale,
    attn_gate,
    final_shift,
    final_scale,
    q_weight,
    k_weight,
    v_weight,
    o_weight,
    out_weight,
    neighbour_mask,
    blend_weight,
):
    mask = neighbour_mask.reshape(4)
    tile, top, rest, near, body, side = call(
        pack_kernel,
        [((n, D), BF16) for n in (TILE, TOP, REST, CUT, TILE - CUT, SIDE)],
        latent,
        limit=4 * MB,
        flops=1 << 33,
    )
    east, far = fetch(near, 0, 1), fetch(side, 0, 2)
    east_body = fetch(body, 0, 1)
    west_top, west_rest = fetch(top, 0, -1), fetch(rest, 0, -1)
    north, south = fetch(tile, -1, 0), fetch(tile, 1, 0)
    low = fetch(top, 2, 0)
    q0, k0, v0 = call(
        own_kernel,
        [((TILE, AD), BF16)] * 3,
        tile, attn_scale, attn_shift, q_weight, k_weight, v_weight,
        limit=8 * MB,
    )
    to_up, to_down, to_twice = call(
        relay_kernel,
        [((n, D), BF16) for n in (RELAY, SIDE, CORNER)],
        east, far, west_top,
        limit=4 * MB,
    )
    relayed = fetch(to_up, 1, 0)
    north_side = fetch(to_down, -1, 0)
    low_corner = fetch(to_twice, 2, 0)
    q1, k1, v1 = call(
        mid_kernel,
        [((n, AD), BF16) for n in (SIDE + TOP, EARLY - TILE, EARLY - TILE)],
        east, south, far, north, low, west_top, east_body,
        attn_scale, attn_shift, q_weight, k_weight, v_weight,
        scratch=[((EARLY - TILE, D), BF16)],
        limit=12 * MB,
    )
    cover, pick, out_t = jnp.asarray(coverage()), jnp.asarray(query_columns()), out_weight.T
    spill_e, spill_s, spill_c, keys, vals = call(
        spill_kernel,
        [((n, LANES), F32) for n in (SIDE, TOP, CORNER)] + [((KEYS, AD), BF16)] * 2,
        mask, cover, pick, east, south,
        relayed, north_side, west_rest, low_corner,
        k0, v0, q1, k1, v1,
        attn_scale, attn_shift, attn_gate, final_scale, final_shift,
        q_weight, k_weight, v_weight, o_weight, out_t, blend_weight,
        scratch=[((LATE, D), BF16), ((OWN - TILE, AD), BF16), ((OWN - TILE, AD), BF16)],
        smem=1,
        limit=16 * MB,
    )
    left = fetch(spill_e, 0, -1)
    diag = fetch(spill_c, -1, -1)
    upper = fetch(spill_s, -1, 0)
    (kept,) = call(
        kept_kernel,
        [((TILE, LANES), F32)],
        mask, cover, pick, tile, q0, keys, vals,
        attn_gate, final_scale, final_shift, o_weight, out_t, blend_weight,
        scratch=[((TILE, AD), BF16)],
        smem=1,
        limit=16 * MB,
    )
    (out,) = call(blend_kernel, [((TH, TW * P_SIZE), F32)], kept, left, upper, diag, limit=4 * MB)
    return out


def solution(mesh):
    in_specs = (
        P("row", "col", None),
        P(),
        P(),
        P(),
        P(),
        P(),
        P(),
        P(),
        P(),
        P(),
        P(),
        P("row", "col", None),
        P("row", "col"),
    )
    out_specs = P("row", "col")
    return jax.shard_map(block, mesh=mesh, in_specs=in_specs, out_specs=out_specs, check_vma=False)
```
